32 devices in a mesh: sp: 8 (over z, x), tp: 4 (over y, core).
Axes of the slice: x: 2, y: 2, z: 4, core: 2. Of those that a mesh axis runs over, the one named last changes fastest.
Arguments:
- prefill_keys: bfloat16 [2, 8, 512, 8, 128], P(None, None, 'sp', 'tp'), may hold values from -6 to 6
- prefill_values: bfloat16 [2, 8, 512, 8, 128], P(None, None, 'sp', 'tp'), may hold values from -6 to 6
- prompt_lengths: int32 [8], replicated, may hold values from 1 to 512, 2048 in all
- destination: int32 [8], replicated, may hold values from 0 to 7, each once
- page_table: int32 [8, 32], P('sp'), may hold values from 0 to 31, as said below
- queries: bfloat16 [2, 8, 64, 128], P(None, 'sp', 'tp'), may hold values from -6 to 6
Outputs:
- key_pages: bfloat16 [2, 256, 16, 8, 128], P(None, 'sp', None, 'tp')
- value_pages: bfloat16 [2, 256, 16, 8, 128], P(None, 'sp', None, 'tp')
- attended: bfloat16 [2, 8, 64, 128], P(None, 'sp')
The draws below stay inside these ranges and needn't reach their ends.
Inputs may be any that keep to these rules, and one draw needn't show every extreme that they name: `destination`: each slot is named by exactly one prompt; slot s is held by sp index s // 1. `page_table`: the rows of the 1 slots of one sp index together name each of that index's 1 times 32 local pool pages exactly once.
All inputs are finite; a program needn't handle non-finite values.
Results may differ from the reference program's by a relative error of at most 0.0085.
Values may be sent and summed in bfloat16 or wider, within the bound.
A program may use at most 128 MiB of HBM per device.

```python
import math
import jax
import jax.numpy as jnp
import numpy as np
from jax import lax

QH = 64
KVH = 8
HD = 128
LAYERS = 2
PAGE = 16
PROM_DEV = 1
PROMPTS = 8
MAXLEN = 512
PAGES = 32
POOL = 256


def draw_page_table(key, part):
    devices = PROMPTS // PROM_DEV
    key_list = jax.random.split(key, devices)
    orders = jax.vmap(lambda sub_key: jax.random.permutation(sub_key, PROM_DEV * PAGES))(key_list)
    return orders.reshape(PROMPTS, PAGES).astype(jnp.int32)


def block_levels(stream_key, shape, pieces, least, top_value):
    def one(position, parts):
        draws = jax.random.uniform(jax.random.fold_in(jax.random.fold_in(stream_key, 6), position), (parts,), jnp.float32, least / len(pieces), top_value / len(pieces))
        return jnp.repeat(jnp.exp(draws), shape[position] // parts).reshape((-1,) + (1,) * (len(shape) - position - 1))

    gain = one(*pieces[0])
    for cut in pieces[1:]:
        gain = gain * one(*cut)
    return gain


def split_up(count, total, limit, skew):
    portions = [(1 << 20) // math.isqrt(rank ** skew) + 1 for rank in range(2, count + 1)]
    spare, holding = total - limit - (count - 1), [1] * (count - 1)
    while spare > 0:
        movable = [i for i in range(count - 1) if holding[i] < limit]
        whole, budget = sum([portions[i] for i in movable]), spare
        for i in movable:
            extra = min(limit - holding[i], max(1, budget * portions[i] // whole), spare)
            holding[i] = holding[i] + extra
            spare = spare - extra
    return np.array([limit] + holding)


def ragged_sizes(key, number_of, total, bound, lean):
    if number_of == 2:
        one = jax.random.randint(key, (), max(1, total - bound), min(bound, total - 1) + 1)
        return jnp.stack([one, total - one])
    tallies = jnp.asarray(split_up(number_of, total, bound, lean), jnp.int32)
    twos = (number_of - 1) // 2
    donor, taker = tallies[1:1 + 2 * twos:2], tallies[2:2 + 2 * twos:2]
    room = jnp.minimum(donor - 1, bound - taker)
    moved = jax.random.randint(jax.random.fold_in(key, 1), (twos,), 0, 1 << 20) % (room + 1)
    tallies = tallies.at[1:1 + 2 * twos:2].set(donor - moved).at[2:2 + 2 * twos:2].set(taker + moved)
    return tallies[jax.random.permutation(jax.random.fold_in(key, 2), number_of)]


def scatter_about(key, shape, deviation, reach, cuts=(), kind=jnp.bfloat16):
    values = jax.random.normal(key, shape, jnp.float32) * deviation
    if len(cuts) > 0:
        values = block_levels(key, shape, cuts, -0.22, 0.18) * values
    return jnp.clip(values, min=-reach, max=reach).astype(kind)


def setup_inputs(seed: int = 0) -> dict:
    arg_keys = jax.random.split(jax.random.key(seed), 7)
    return {
        "prefill_keys": scatter_about(arg_keys[0], (LAYERS, PROMPTS, MAXLEN, KVH, HD), 1.0, 6.0, ((2, 8), (3, 4))),
        "prefill_values": scatter_about(arg_keys[1], (LAYERS, PROMPTS, MAXLEN, KVH, HD), 1.0, 6.0, ((2, 8), (3, 4))),
        "prompt_lengths": ragged_sizes(arg_keys[2], PROMPTS, PROMPTS * MAXLEN // 2, MAXLEN, 1).astype(jnp.int32),
        "destination": jax.random.permutation(arg_keys[3], PROMPTS).astype(jnp.int32),
        "page_table": draw_page_table(jax.random.fold_in(arg_keys[6], 71), 0),
        "queries": scatter_about(arg_keys[5], (LAYERS, PROMPTS, QH, HD), 1.0, 6.0, ((1, 8), (2, 4))),
    }


def reference(prefill_keys, prefill_values, prompt_lengths, destination, page_table, queries):
    holder = jnp.zeros((PROMPTS,), jnp.int32).at[destination].set(jnp.arange(PROMPTS, dtype=jnp.int32))
    slot_len = prompt_lengths[holder]
    positions = jnp.arange(MAXLEN, dtype=jnp.int32)
    inside = positions[None, :] < slot_len[:, None]
    seq_keys = jnp.where(inside[None, :, :, None, None], prefill_keys[:, holder], 0).astype(jnp.bfloat16)
    seq_values = jnp.where(inside[None, :, :, None, None], prefill_values[:, holder], 0).astype(jnp.bfloat16)
    device_of = jnp.arange(PROMPTS, dtype=jnp.int32) // PROM_DEV
    global_page = (device_of[:, None] * (PROM_DEV * PAGES) + page_table).reshape(-1)
    key_blocks = seq_keys.reshape(LAYERS, POOL, PAGE, KVH, HD)
    value_blocks = seq_values.reshape(LAYERS, POOL, PAGE, KVH, HD)
    key_pages = jnp.zeros(key_blocks.shape, jnp.bfloat16).at[:, global_page].set(key_blocks)
    value_pages = jnp.zeros(value_blocks.shape, jnp.bfloat16).at[:, global_page].set(value_blocks)
    groups = QH // KVH
    score_scale = HD ** -0.5

    def one_layer(operands):
        layer_q, layer_k, layer_v = operands
        grouped = layer_q.astype(jnp.float32).reshape(PROMPTS, KVH, groups, HD)
        scores = jnp.einsum("pkgd,ptkd->pkgt", grouped, layer_k.astype(jnp.float32)) * score_scale
        scores = jnp.where(inside[:, None, None, :], scores, -1e30)
        weights = jax.nn.softmax(scores, axis=-1)
        output = jnp.einsum("pkgt,ptkd->pkgd", weights, layer_v.astype(jnp.float32))
        return output.reshape(PROMPTS, QH, HD).astype(jnp.bfloat16)

    attended = lax.map(one_layer, (queries, seq_keys, seq_values))
    return key_pages, value_pages, attended
```

```python
import functools

import jax
import jax.numpy as jnp
from jax import lax
from jax.experimental import pallas as pl
from jax.experimental.pallas import tpu as pltpu
from jax.sharding import PartitionSpec as P

MESH = pl.DeviceIdType.MESH


def partner(me, step, n, way=1):
    if n & (n - 1):
        return lax.rem(me + way * step + n, n)
    total, bit = 0, 1
    while bit < n:
        total = total + ((me // bit + step // bit) % 2) * bit
        bit *= 2
    return total


def kernel(
    sp_size, tp_size, page_size,
    lengths, destination, table, queries, keys_in, values_in,
    key_pages, value_pages, attended,
    fetched, outbox, inboxes, staged, heads_out, inverse,
    fetch_sem, send_sem, recv_sem, store_sem, head_send_sem, head_recv_sem,
):
    layers, prompts, rows, head_size = keys_in.shape
    per_block, page_rows = outbox.shape[3], outbox.shape[4]
    heads_here = page_rows // page_size
    pages = table.shape[1]
    query_heads = queries.shape[1]
    me, row = lax.axis_index("sp"), lax.axis_index("tp")

    def head_copy(layer, step):
        other = lax.rem(row + step, tp_size)
        return pltpu.make_async_remote_copy(
            src_ref=heads_out.at[layer, row],
            dst_ref=heads_out.at[layer, row],
            send_sem=head_send_sem.at[layer, step],
            recv_sem=head_recv_sem.at[layer, step],
            device_id={"tp": other},
            device_id_type=MESH,
        )

    def block_copy(layer, step):
        other = partner(me, step, sp_size)
        return pltpu.make_async_remote_copy(
            src_ref=outbox.at[layer, other],
            dst_ref=inboxes[layer].at[me],
            send_sem=send_sem.at[layer, step],
            recv_sem=recv_sem.at[layer, step],
            device_id={"sp": other},
            device_id_type=MESH,
        )

    fetches = []
    for layer in range(layers):
        for kind, source in enumerate((keys_in, values_in)):
            fetch = pltpu.make_async_copy(
                source.at[layer], fetched.at[layer, kind], fetch_sem.at[layer, kind]
            )
            fetch.start()
            fetches.append(fetch)

    barrier = pltpu.get_barrier_semaphore()

    def greet_sp(step, carry):
        pl.semaphore_signal(
            barrier, inc=1, device_id={"sp": partner(me, step, sp_size)}, device_id_type=MESH
        )
        return carry

    lax.fori_loop(1, sp_size, greet_sp, 0)
    for step in range(1, tp_size):
        pl.semaphore_signal(
            barrier, inc=1, device_id={"tp": lax.rem(row + step, tp_size)}, device_id_type=MESH
        )

    def holder_of(slot):
        def look(prompt, found):
            return jnp.where(destination[prompt] == slot, prompt, found)

        return lax.fori_loop(0, prompts, look, jnp.int32(0), unroll=prompts <= 8)

    my_len = lengths[holder_of(me)]
    for fetch in fetches:
        fetch.wait()

    def fill(step, carry):
        other = partner(me, step, sp_size)
        held = holder_of(other)
        for layer in range(layers):
            for kind in range(2):
                block = fetched[layer, kind, held]
                outbox[layer, other, kind] = block.reshape(per_block, page_rows, head_size)
        return carry

    lax.fori_loop(1, sp_size, fill, 0)
    own = holder_of(me)
    for layer in range(layers):
        for kind in range(2):
            block = fetched[layer, kind, own]
            inboxes[layer][me, kind] = block.reshape(per_block, page_rows, head_size)

    pl.semaphore_wait(barrier, sp_size - 1 + tp_size - 1)

    for layer in range(layers):
        def send(step, carry):
            block_copy(layer, step).start()
            return carry

        lax.fori_loop(1, sp_size, send, 0)

    def invert(page, carry):
        def look(position, found):
            return jnp.where(table[0, position] == page, position, found)

        inverse[page] = lax.fori_loop(0, pages, look, jnp.int32(0), unroll=pages <= 32)
        return carry

    lax.fori_loop(0, pages, invert, 0)

    groups = query_heads // heads_here
    shape = (query_heads, rows)
    column = lax.broadcasted_iota(jnp.int32, shape, 1)
    column_head, column_token = column % heads_here, column // heads_here
    same_head = lax.broadcasted_iota(jnp.int32, shape, 0) // groups == column_head
    page_token = lax.broadcasted_iota(jnp.int32, (page_rows, head_size), 0) // heads_here
    scale = head_size ** (-0.5)
    tokens = rows // heads_here

    stores = []
    for layer in range(layers):
        asked = queries[layer]

        def attend(step, carry):
            top, total, mixed = carry
            source = partner(me, step, sp_size, -1)

            @pl.when(step > 0)
            def _():
                block_copy(layer, step).wait_recv()

            block_keys = inboxes[layer][source, 0].reshape(rows, head_size)
            block_values = inboxes[layer][source, 1].reshape(rows, head_size)
            scores = lax.dot_general(
                asked, block_keys, (((1,), (1,)), ((), ())), preferred_element_type=jnp.float32
            ) * scale
            seen = same_head & (column_token + source * tokens < my_len)
            scores = jnp.where(seen, scores, -1e30)
            new_top = jnp.maximum(top, jnp.max(scores, axis=1, keepdims=True))
            fade = jnp.exp(top - new_top)
            weights = jnp.exp(scores - new_top)
            high = weights.astype(jnp.bfloat16)
            low = (weights - high.astype(jnp.float32)).astype(jnp.bfloat16)
            part = jnp.dot(high, block_values, preferred_element_type=jnp.float32) + jnp.dot(
                low, block_values, preferred_element_type=jnp.float32
            )
            total = total * fade + jnp.sum(weights, axis=1, keepdims=True)
            return new_top, total, mixed * fade + part

        _, total, mixed = lax.fori_loop(
            0, sp_size, attend,
            (
                jnp.full((query_heads, 1), -1e30, jnp.float32),
                jnp.zeros((query_heads, 1), jnp.float32),
                jnp.zeros((query_heads, head_size), jnp.float32),
            ),
        )
        heads_out[layer, row] = (mixed / total).astype(jnp.bfloat16)

        def place(page, carry):
            position = inverse[page]
            source, within = position // per_block, position % per_block
            inside = page_token + position * page_size < my_len
            for kind in range(2):
                content = inboxes[layer][source, kind, within]
                staged[layer, kind, page] = jnp.where(inside, content, jnp.zeros_like(content))
            return carry

        lax.fori_loop(0, pages, place, 0)
        for step in range(1, tp_size):
            head_copy(layer, step).start()
        for kind, target in enumerate((key_pages, value_pages)):
            store = pltpu.make_async_copy(
                staged.at[layer, kind], target.at[layer], store_sem.at[layer, kind]
            )
            store.start()
            stores.append(store)

    for layer in range(layers):
        def sent(step, carry):
            block_copy(layer, step).wait_send()
            return carry

        lax.fori_loop(1, sp_size, sent, 0)
    for store in stores:
        store.wait()
    for layer in range(layers):
        for step in range(1, tp_size):
            head_copy(layer, step).wait()
        attended[layer] = heads_out[layer].reshape(tp_size * query_heads, head_size)


def local(sp_size, tp_size, prefill_keys, prefill_values, prompt_lengths, destination, page_table, queries):
    layers, prompts, tokens, heads_here, head_size = prefill_keys.shape
    slots_here, pages = page_table.shape
    query_heads = queries.shape[2]
    page_size = tokens * sp_size // pages
    rows, page_rows = tokens * heads_here, page_size * heads_here
    per_block = tokens // page_size
    assert slots_here == 1 and per_block * page_size == tokens
    flat = (layers, prompts, rows, head_size)
    paged = jax.ShapeDtypeStruct((layers, pages, page_rows, head_size), prefill_keys.dtype)
    everywhere = pl.BlockSpec(memory_space=pl.ANY)
    scalars = pl.BlockSpec(memory_space=pltpu.SMEM)
    vectors = pl.BlockSpec(memory_space=pltpu.VMEM)
    boxes = (layers, sp_size, 2, per_block, page_rows, head_size)
    kind = prefill_keys.dtype
    dma = pltpu.SemaphoreType.DMA
    key_pages, value_pages, attended = pl.pallas_call(
        functools.partial(kernel, sp_size, tp_size, page_size),
        out_shape=(
            paged,
            paged,
            jax.ShapeDtypeStruct((layers, tp_size * query_heads, head_size), jnp.bfloat16),
        ),
        in_specs=[scalars, scalars, scalars, vectors, everywhere, everywhere],
        out_specs=(everywhere, everywhere, vectors),
        scratch_shapes=[
            pltpu.VMEM((layers, 2, prompts, rows, head_size), kind),
            pltpu.VMEM(boxes, kind),
            (pltpu.VMEM(boxes[1:], kind),) * layers,
            pltpu.VMEM((layers, 2, pages, page_rows, head_size), kind),
            pltpu.VMEM((layers, tp_size, query_heads, head_size), jnp.bfloat16),
            pltpu.SMEM((pages,), jnp.int32),
            dma((layers, 2)),
            dma((layers, sp_size)),
            dma((layers, sp_size)),
            dma((layers, 2)),
            dma((layers, tp_size)),
            dma((layers, tp_size)),
        ],
        compiler_params=pltpu.CompilerParams(collective_id=0, has_side_effects=True),
    )(
        prompt_lengths,
        destination,
        page_table,
        queries.reshape(layers, query_heads, head_size),
        prefill_keys.reshape(flat),
        prefill_values.reshape(flat),
    )
    shape = (layers, pages, page_size, heads_here, head_size)
    return (
        key_pages.reshape(shape),
        value_pages.reshape(shape),
        attended.reshape(layers, 1, tp_size * query_heads, head_size),
    )


def solution(mesh):
    placed = (
        P(None, None, "sp", "tp", None),
        P(None, None, "sp", "tp", None),
        P(),
        P(),
        P("sp", None),
        P(None, "sp", "tp", None),
    )
    return jax.shard_map(
        functools.partial(local, mesh.shape["sp"], mesh.shape["tp"]),
        mesh=mesh,
        in_specs=placed,
        out_specs=(
            P(None, "sp", None, "tp", None),
            P(None, "sp", None, "tp", None),
            P(None, "sp", None, None),
        ),
        check_vma=False,
    )
```

```python
import functools

import jax
import jax.numpy as jnp
from jax import lax
from jax.experimental import pallas as pl
from jax.experimental.pallas import tpu as pltpu
from jax.sharding import PartitionSpec as P

MESH = pl.DeviceIdType.MESH


def partner(me, step, n, way=1):
    if n & (n - 1):
        return lax.rem(me + way * step + n, n)
    total, bit = 0, 1
    while bit < n:
        total = total + ((me // bit + step // bit) % 2) * bit
        bit *= 2
    return total


def turn(me, step, n):
    if n & (n - 1) or n < 4:
        return step
    outer = (me // (n // 4) + me // (n // 2) + 1) % 2
    crossing = step // (n // 2)
    return step + crossing * ((step + outer * (n // 4)) % (n // 2) + n // 2 - step)


def kernel(
    sp_size, tp_size, page_size,
    lengths, destination, table, queries, keys_in, values_in,
    key_pages, value_pages, attended,
    fetched, outbox, inboxes, heads_out, inverse,
    fetch_sem, send_sem, recv_sem, head_send_sem, head_recv_sem,
):
    layers, prompts, rows, head_size = keys_in.shape
    per_block, page_rows = outbox.shape[3], outbox.shape[4]
    heads_here = page_rows // page_size
    pages = table.shape[1]
    query_heads = queries.shape[1]
    me, row = lax.axis_index("sp"), lax.axis_index("tp")

    def head_copy(layer, step):
        other = lax.rem(row + step, tp_size)
        return pltpu.make_async_remote_copy(
            src_ref=heads_out.at[layer, row],
            dst_ref=heads_out.at[layer, row],
            send_sem=head_send_sem.at[layer, step],
            recv_sem=head_recv_sem.at[layer, step],
            device_id={"tp": other},
            device_id_type=MESH,
        )

    def block_copy(layer, step):
        other = partner(me, step, sp_size)
        return pltpu.make_async_remote_copy(
            src_ref=outbox.at[layer, other],
            dst_ref=inboxes[layer].at[me],
            send_sem=send_sem.at[layer, step],
            recv_sem=recv_sem.at[layer, step],
            device_id={"sp": other},
            device_id_type=MESH,
        )

    fetches = []
    for layer in range(layers):
        for kind, source in enumerate((keys_in, values_in)):
            fetch = pltpu.make_async_copy(
                source.at[layer], fetched.at[layer, kind], fetch_sem.at[layer, kind]
            )
            fetch.start()
            fetches.append(fetch)

    barrier = pltpu.get_barrier_semaphore()

    def greet_sp(step, carry):
        pl.semaphore_signal(
            barrier, inc=1, device_id={"sp": partner(me, step, sp_size)}, device_id_type=MESH
        )
        return carry

    lax.fori_loop(1, sp_size, greet_sp, 0)
    for step in range(1, tp_size):
        pl.semaphore_signal(
            barrier, inc=1, device_id={"tp": lax.rem(row + step, tp_size)}, device_id_type=MESH
        )

    def holder_of(slot):
        def look(prompt, found):
            return jnp.where(destination[prompt] == slot, prompt, found)

        return lax.fori_loop(0, prompts, look, jnp.int32(0), unroll=prompts <= 8)

    my_len = lengths[holder_of(me)]
    for fetch in fetches:
        fetch.wait()

    def fill(step, carry):
        other = partner(me, step, sp_size)
        held = holder_of(other)
        for layer in range(layers):
            for kind in range(2):
                block = fetched[layer, kind, held]
                outbox[layer, other, kind] = block.reshape(per_block, page_rows, head_size)
        return carry

    lax.fori_loop(1, sp_size, fill, 0)
    own = holder_of(me)
    for layer in range(layers):
        for kind in range(2):
            block = fetched[layer, kind, own]
            inboxes[layer][me, kind] = block.reshape(per_block, page_rows, head_size)

    pl.semaphore_wait(barrier, sp_size - 1 + tp_size - 1)

    for layer in range(layers):
        def send(step, carry):
            block_copy(layer, turn(me, step, sp_size)).start()
            return carry

        lax.fori_loop(1, sp_size, send, 0)

    def invert(page, carry):
        def look(position, found):
            return jnp.where(table[0, position] == page, position, found)

        inverse[page] = lax.fori_loop(0, pages, look, jnp.int32(0), unroll=pages <= 32)
        return carry

    lax.fori_loop(0, pages, invert, 0)

    groups = query_heads // heads_here
    shape = (query_heads, rows)
    column = lax.broadcasted_iota(jnp.int32, shape, 1)
    column_head, column_token = column % heads_here, column // heads_here
    same_head = lax.broadcasted_iota(jnp.int32, shape, 0) // groups == column_head
    page_token = lax.broadcasted_iota(jnp.int32, (page_rows, head_size), 0) // heads_here
    scale = head_size ** (-0.5)
    tokens = rows // heads_here

    for layer in range(layers):
        asked = queries[layer]

        def attend(step, carry):
            top, total, mixed = carry
            step = turn(me, step, sp_size)
            source = partner(me, step, sp_size, -1)

            @pl.when(step > 0)
            def _():
                block_copy(layer, step).wait_recv()

            block_keys = inboxes[layer][source, 0].reshape(rows, head_size)
            block_values = inboxes[layer][source, 1].reshape(rows, head_size)
            scores = lax.dot_general(
                asked, block_keys, (((1,), (1,)), ((), ())), preferred_element_type=jnp.float32
            ) * scale
            seen = same_head & (column_token + source * tokens < my_len)
            scores = jnp.where(seen, scores, -1e30)
            new_top = jnp.maximum(top, jnp.max(scores, axis=1, keepdims=True))
            fade = jnp.exp(top - new_top)
            weights = jnp.exp(scores - new_top)
            high = weights.astype(jnp.bfloat16)
            low = (weights - high.astype(jnp.float32)).astype(jnp.bfloat16)
            part = jnp.dot(high, block_values, preferred_element_type=jnp.float32) + jnp.dot(
                low, block_values, preferred_element_type=jnp.float32
            )
            total = total * fade + jnp.sum(weights, axis=1, keepdims=True)
            return new_top, total, mixed * fade + part

        _, total, mixed = lax.fori_loop(
            0, sp_size, attend,
            (
                jnp.full((query_heads, 1), -1e30, jnp.float32),
                jnp.zeros((query_heads, 1), jnp.float32),
                jnp.zeros((query_heads, head_size), jnp.float32),
            ),
        )
        heads_out[layer, row] = (mixed / total).astype(jnp.bfloat16)

        def place(page, carry):
            position = inverse[page]
            source, within = position // per_block, position % per_block
            inside = page_token + position * page_size < my_len
            for kind, target in enumerate((key_pages, value_pages)):
                content = inboxes[layer][source, kind, within]
                target[layer, page] = jnp.where(inside, content, jnp.zeros_like(content))
            return carry

        early = pages // 8
        lax.fori_loop(0, early, place, 0, unroll=early <= 4)
        for step in range(1, tp_size):
            head_copy(layer, step).start()
        lax.fori_loop(early, pages, place, 0, unroll=4)

    for layer in range(layers):
        def sent(step, carry):
            block_copy(layer, step).wait_send()
            return carry

        lax.fori_loop(1, sp_size, sent, 0)
    for layer in range(layers):
        for step in range(1, tp_size):
            head_copy(layer, step).wait()
        attended[layer] = heads_out[layer].reshape(tp_size * query_heads, head_size)


def write_out(*refs):
    sources, targets, sems = refs[:3], refs[3:6], refs[6]
    copies = [
        pltpu.make_async_copy(sources[i], targets[i], sems.at[i]) for i in range(3)
    ]
    for copy in copies:
        copy.start()
    for copy in copies:
        copy.wait()


def local(sp_size, tp_size, prefill_keys, prefill_values, prompt_lengths, destination, page_table, queries):
    layers, prompts, tokens, heads_here, head_size = prefill_keys.shape
    slots_here, pages = page_table.shape
    query_heads = queries.shape[2]
    page_size = tokens * sp_size // pages
    rows, page_rows = tokens * heads_here, page_size * heads_here
    per_block = tokens // page_size
    assert slots_here == 1 and per_block * page_size == tokens
    flat = (layers, prompts, rows, head_size)
    paged = (layers, pages, page_rows, head_size)
    shapes = (paged, paged, (layers, tp_size * query_heads, head_size))
    everywhere = pl.BlockSpec(memory_space=pl.ANY)
    scalars = pl.BlockSpec(memory_space=pltpu.SMEM)
    vectors = pl.BlockSpec(memory_space=pltpu.VMEM)
    boxes = (layers, sp_size, 2, per_block, page_rows, head_size)
    kind = prefill_keys.dtype
    dma = pltpu.SemaphoreType.DMA
    grant = min(60 * 1024 * 1024, 67043328 - 2 * prefill_keys.size * kind.itemsize - (1 << 20))
    results = pl.pallas_call(
        functools.partial(kernel, sp_size, tp_size, page_size),
        out_shape=tuple(pltpu.VMEM(shape, kind) for shape in shapes),
        in_specs=[scalars, scalars, scalars, vectors, everywhere, everywhere],
        out_specs=(vectors, vectors, vectors),
        scratch_shapes=[
            pltpu.VMEM((layers, 2, prompts, rows, head_size), kind),
            pltpu.VMEM(boxes, kind),
            (pltpu.VMEM(boxes[1:], kind),) * layers,
            pltpu.VMEM((layers, tp_size, query_heads, head_size), jnp.bfloat16),
            pltpu.SMEM((pages,), jnp.int32),
            dma((layers, 2)),
            dma((layers, sp_size)),
            dma((layers, sp_size)),
            dma((layers, tp_size)),
            dma((layers, tp_size)),
        ],
        compiler_params=pltpu.CompilerParams(
            collective_id=0, has_side_effects=True, vmem_limit_bytes=grant
        ),
    )(
        prompt_lengths,
        destination,
        page_table,
        queries.reshape(layers, query_heads, head_size),
        prefill_keys.reshape(flat),
        prefill_values.reshape(flat),
    )
    key_pages, value_pages, attended = pl.pallas_call(
        write_out,
        out_shape=tuple(jax.ShapeDtypeStruct(shape, kind) for shape in shapes),
        in_specs=[vectors] * 3,
        out_specs=(everywhere,) * 3,
        scratch_shapes=[dma((3,))],
        compiler_params=pltpu.CompilerParams(vmem_limit_bytes=1 << 20),
    )(*(pltpu.with_memory_space_constraint(x, pltpu.VMEM) for x in results))
    shape = (layers, pages, page_size, heads_here, head_size)
    return (
        key_pages.reshape(shape),
        value_pages.reshape(shape),
        attended.reshape(layers, 1, tp_size * query_heads, head_size),
    )


def solution(mesh):
    placed = (
        P(None, None, "sp", "tp", None),
        P(None, None, "sp", "tp", None),
        P(),
        P(),
        P("sp", None),
        P(None, "sp", "tp", None),
    )
    return jax.shard_map(
        functools.partial(local, mesh.shape["sp"], mesh.shape["tp"]),
        mesh=mesh,
        in_specs=placed,
        out_specs=(
            P(None, "sp", None, "tp", None),
            P(None, "sp", None, "tp", None),
            P(None, "sp", None, None),
        ),
        check_vma=False,
    )
```

```python
import functools

import jax
import jax.numpy as jnp
from jax import lax
from jax.experimental import pallas as pl
from jax.experimental.pallas import tpu as pltpu
from jax.sharding import PartitionSpec as P

MESH = pl.DeviceIdType.MESH


def partner(me, step, n, way=1):
    if n & (n - 1):
        return lax.rem(me + way * step + n, n)
    total, bit = 0, 1
    while bit < n:
        total = total + ((me // bit + step // bit) % 2) * bit
        bit *= 2
    return total


def staged(n):
    return n >= 4 and not n & (n - 1)


def turn(me, step, n, last):
    if not staged(n):
        return step
    inner = (me // (n // 4) + me // (n // 2)) % 2
    swap = 1 - inner if last else inner
    crossing = step // (n // 2)
    return step + crossing * ((step + swap * (n // 4)) % (n // 2) + n // 2 - step)


def kernel(
    sp_size, tp_size, page_size,
    lengths, destination, table, queries, keys_in, values_in,
    key_pages, value_pages, attended,
    fetched, outbox, inboxes, heads_out, inverse,
    fetch_sem, send_sem, recv_sem, head_send_sem, head_recv_sem, far_sem,
):
    layers, prompts, rows, head_size = keys_in.shape
    per_block, page_rows = outbox.shape[3], outbox.shape[4]
    heads_here = page_rows // page_size
    pages = table.shape[1]
    query_heads = queries.shape[1]
    me, row = lax.axis_index("sp"), lax.axis_index("tp")

    def head_copy(layer, step):
        other = lax.rem(row + step, tp_size)
        return pltpu.make_async_remote_copy(
            src_ref=heads_out.at[layer, row],
            dst_ref=heads_out.at[layer, row],
            send_sem=head_send_sem.at[layer, step],
            recv_sem=head_recv_sem.at[layer, step],
            device_id={"tp": other},
            device_id_type=MESH,
        )

    def block_copy(layer, step):
        other = partner(me, step, sp_size)
        return pltpu.make_async_remote_copy(
            src_ref=outbox.at[layer, other],
            dst_ref=inboxes[layer].at[me],
            send_sem=send_sem.at[layer, step],
            recv_sem=recv_sem.at[layer, step],
            device_id={"sp": other},
            device_id_type=MESH,
        )

    fetches = []
    for layer in range(layers):
        for kind, source in enumerate((keys_in, values_in)):
            fetch = pltpu.make_async_copy(
                source.at[layer], fetched.at[layer, kind], fetch_sem.at[layer, kind]
            )
            fetch.start()
            fetches.append(fetch)

    barrier = pltpu.get_barrier_semaphore()

    def greet_sp(step, carry):
        pl.semaphore_signal(
            barrier, inc=1, device_id={"sp": partner(me, step, sp_size)}, device_id_type=MESH
        )
        return carry

    half, quarter = sp_size // 2, sp_size // 4
    split = staged(sp_size)
    if split:
        place_in_line, place_in_quarter = me // quarter, me % quarter
        inner = (place_in_line + me // half) % 2
        lax.fori_loop(1, half, greet_sp, 0)

        @pl.when(inner == 1)
        def _():
            lax.fori_loop(half + quarter, sp_size, greet_sp, 0)

        greeted = half - 1 + inner * quarter
    else:
        lax.fori_loop(1, sp_size, greet_sp, 0)
        greeted = sp_size - 1
    for step in range(1, tp_size):
        pl.semaphore_signal(
            barrier, inc=1, device_id={"tp": lax.rem(row + step, tp_size)}, device_id_type=MESH
        )

    def holder_of(slot):
        def look(prompt, found):
            return jnp.where(destination[prompt] == slot, prompt, found)

        return lax.fori_loop(0, prompts, look, jnp.int32(0), unroll=prompts <= 8)

    my_len = lengths[holder_of(me)]
    for fetch in fetches:
        fetch.wait()

    def fill(step, carry):
        other = partner(me, step, sp_size)
        held = holder_of(other)
        for layer in range(layers):
            for kind in range(2):
                block = fetched[layer, kind, held]
                outbox[layer, other, kind] = block.reshape(per_block, page_rows, head_size)
        return carry

    lax.fori_loop(1, sp_size, fill, 0)
    own = holder_of(me)
    for layer in range(layers):
        for kind in range(2):
            block = fetched[layer, kind, own]
            inboxes[layer][me, kind] = block.reshape(per_block, page_rows, head_size)

    pl.semaphore_wait(barrier, greeted + tp_size - 1)

    def send_steps(layer, first, stop):
        def send(step, carry):
            block_copy(layer, turn(me, step, sp_size, layer == layers - 1 and layer > 0)).start()
            return carry

        lax.fori_loop(first, stop, send, 0)

    def pass_on(level, line):
        pl.semaphore_signal(
            far_sem.at[level], inc=1,
            device_id={"sp": line * quarter + place_in_quarter}, device_id_type=MESH,
        )

    if split:
        outward, inward = (place_in_line // 2) * 3, 3 - place_in_line

        @pl.when(inner == 1)
        def _():
            pass_on(0, inward)
            pass_on(0, outward)
            send_steps(0, 1, half + quarter)
            pl.semaphore_wait(far_sem.at[0], 1)
            pass_on(1, outward)
            send_steps(0, half + quarter, sp_size)

        @pl.when(inner == 0)
        def _():
            send_steps(0, 1, half)
            pl.semaphore_wait(far_sem.at[0], 1)
            send_steps(0, half, half + quarter)
            pl.semaphore_wait(far_sem.at[1], 1)
            send_steps(0, half + quarter, sp_size)
    else:
        send_steps(0, 1, sp_size)
    for layer in range(1, layers):
        send_steps(layer, 1, sp_size)

    def invert(page, carry):
        def look(position, found):
            return jnp.where(table[0, position] == page, position, found)

        inverse[page] = lax.fori_loop(0, pages, look, jnp.int32(0), unroll=pages <= 32)
        return carry

    lax.fori_loop(0, pages, invert, 0)

    groups = query_heads // heads_here
    shape = (query_heads, rows)
    column = lax.broadcasted_iota(jnp.int32, shape, 1)
    column_head, column_token = column % heads_here, column // heads_here
    same_head = lax.broadcasted_iota(jnp.int32, shape, 0) // groups == column_head
    page_token = lax.broadcasted_iota(jnp.int32, (page_rows, head_size), 0) // heads_here
    scale = head_size ** (-0.5)
    tokens = rows // heads_here

    for layer in range(layers):
        asked = queries[layer]

        def attend(step, carry):
            top, total, mixed = carry
            step = turn(me, step, sp_size, layer == layers - 1 and layer > 0)
            source = partner(me, step, sp_size, -1)

            @pl.when(step > 0)
            def _():
                block_copy(layer, step).wait_recv()

            block_keys = inboxes[layer][source, 0].reshape(rows, head_size)
            block_values = inboxes[layer][source, 1].reshape(rows, head_size)
            scores = lax.dot_general(
                asked, block_keys, (((1,), (1,)), ((), ())), preferred_element_type=jnp.float32
            ) * scale
            seen = same_head & (column_token + source * tokens < my_len)
            scores = jnp.where(seen, scores, -1e30)
            new_top = jnp.maximum(top, jnp.max(scores, axis=1, keepdims=True))
            fade = jnp.exp(top - new_top)
            weights = jnp.exp(scores - new_top)
            high = weights.astype(jnp.bfloat16)
            low = (weights - high.astype(jnp.float32)).astype(jnp.bfloat16)
            part = jnp.dot(high, block_values, preferred_element_type=jnp.float32) + jnp.dot(
                low, block_values, preferred_element_type=jnp.float32
            )
            total = total * fade + jnp.sum(weights, axis=1, keepdims=True)
            return new_top, total, mixed * fade + part

        _, total, mixed = lax.fori_loop(
            0, sp_size, attend,
            (
                jnp.full((query_heads, 1), -1e30, jnp.float32),
                jnp.zeros((query_heads, 1), jnp.float32),
                jnp.zeros((query_heads, head_size), jnp.float32),
            ),
        )
        heads_out[layer, row] = (mixed / total).astype(jnp.bfloat16)

        def place(page, carry):
            position = inverse[page]
            source, within = position // per_block, position % per_block
            inside = page_token + position * page_size < my_len
            for kind, target in enumerate((key_pages, value_pages)):
                content = inboxes[layer][source, kind, within]
                target[layer, page] = jnp.where(inside, content, jnp.zeros_like(content))
            return carry

        early = pages // 8
        lax.fori_loop(0, early, place, 0, unroll=early <= 4)
        for step in range(1, tp_size):
            head_copy(layer, step).start()
        lax.fori_loop(early, pages, place, 0, unroll=4)

    for layer in range(layers):
        def sent(step, carry):
            block_copy(layer, step).wait_send()
            return carry

        lax.fori_loop(1, sp_size, sent, 0)
    for layer in range(layers):
        for step in range(1, tp_size):
            head_copy(layer, step).wait()
        attended[layer] = heads_out[layer].reshape(tp_size * query_heads, head_size)


def write_out(*refs):
    sources, targets, sems = refs[:3], refs[3:6], refs[6]
    copies = [
        pltpu.make_async_copy(sources[i], targets[i], sems.at[i]) for i in range(3)
    ]
    for copy in copies:
        copy.start()
    for copy in copies:
        copy.wait()


def local(sp_size, tp_size, prefill_keys, prefill_values, prompt_lengths, destination, page_table, queries):
    layers, prompts, tokens, heads_here, head_size = prefill_keys.shape
    slots_here, pages = page_table.shape
    query_heads = queries.shape[2]
    page_size = tokens * sp_size // pages
    rows, page_rows = tokens * heads_here, page_size * heads_here
    per_block = tokens // page_size
    assert slots_here == 1 and per_block * page_size == tokens
    flat = (layers, prompts, rows, head_size)
    paged = (layers, pages, page_rows, head_size)
    shapes = (paged, paged, (layers, tp_size * query_heads, head_size))
    everywhere = pl.BlockSpec(memory_space=pl.ANY)
    scalars = pl.BlockSpec(memory_space=pltpu.SMEM)
    vectors = pl.BlockSpec(memory_space=pltpu.VMEM)
    boxes = (layers, sp_size, 2, per_block, page_rows, head_size)
    kind = prefill_keys.dtype
    dma = pltpu.SemaphoreType.DMA
    grant = min(60 * 1024 * 1024, 67043328 - 2 * prefill_keys.size * kind.itemsize - (1 << 20))
    results = pl.pallas_call(
        functools.partial(kernel, sp_size, tp_size, page_size),
        out_shape=tuple(pltpu.VMEM(shape, kind) for shape in shapes),
        in_specs=[scalars, scalars, scalars, vectors, everywhere, everywhere],
        out_specs=(vectors, vectors, vectors),
        scratch_shapes=[
            pltpu.VMEM((layers, 2, prompts, rows, head_size), kind),
            pltpu.VMEM(boxes, kind),
            (pltpu.VMEM(boxes[1:], kind),) * layers,
            pltpu.VMEM((layers, tp_size, query_heads, head_size), jnp.bfloat16),
            pltpu.SMEM((pages,), jnp.int32),
            dma((layers, 2)),
            dma((layers, sp_size)),
            dma((layers, sp_size)),
            dma((layers, tp_size)),
            dma((layers, tp_size)),
            pltpu.SemaphoreType.REGULAR((2,)),
        ],
        compiler_params=pltpu.CompilerParams(
            collective_id=0, has_side_effects=True, vmem_limit_bytes=grant
        ),
    )(
        prompt_lengths,
        destination,
        page_table,
        queries.reshape(layers, query_heads, head_size),
        prefill_keys.reshape(flat),
        prefill_values.reshape(flat),
    )
    key_pages, value_pages, attended = pl.pallas_call(
        write_out,
        out_shape=tuple(jax.ShapeDtypeStruct(shape, kind) for shape in shapes),
        in_specs=[vectors] * 3,
        out_specs=(everywhere,) * 3,
        scratch_shapes=[dma((3,))],
        compiler_params=pltpu.CompilerParams(vmem_limit_bytes=1 << 20),
    )(*(pltpu.with_memory_space_constraint(x, pltpu.VMEM) for x in results))
    shape = (layers, pages, page_size, heads_here, head_size)
    return (
        key_pages.reshape(shape),
        value_pages.reshape(shape),
        attended.reshape(layers, 1, tp_size * query_heads, head_size),
    )


def solution(mesh):
    placed = (
        P(None, None, "sp", "tp", None),
        P(None, None, "sp", "tp", None),
        P(),
        P(),
        P("sp", None),
        P(None, "sp", "tp", None),
    )
    return jax.shard_map(
        functools.partial(local, mesh.shape["sp"], mesh.shape["tp"]),
        mesh=mesh,
        in_specs=placed,
        out_specs=(
            P(None, "sp", None, "tp", None),
            P(None, "sp", None, "tp", None),
            P(None, "sp", None, None),
        ),
        check_vma=False,
    )
```

```python
import functools

import jax
import jax.numpy as jnp
from jax import lax
from jax.experimental import pallas as pl
from jax.experimental.pallas import tpu as pltpu
from jax.sharding import PartitionSpec as P

MESH = pl.DeviceIdType.MESH


def partner(me, step, n, way=1):
    if n & (n - 1):
        return lax.rem(me + way * step + n, n)
    total, bit = 0, 1
    while bit < n:
        total = total + ((me // bit + step // bit) % 2) * bit
        bit *= 2
    return total


def staged(n):
    return n >= 4 and not n & (n - 1)


def turn(me, step, n, last):
    if not staged(n):
        return step
    inner = (me // (n // 4) + me // (n // 2)) % 2
    swap = 1 - inner if last else inner
    crossing = step // (n // 2)
    return step + crossing * ((step + swap * (n // 4)) % (n // 2) + n // 2 - step)


def kernel(
    sp_size, tp_size, page_size,
    lengths, destination, table, queries, keys_in, values_in,
    key_pages, value_pages, attended,
    fetched, outbox, inboxes, heads_out, inverse,
    fetch_sem, send_sem, recv_sem, head_send_sem, head_recv_sem, far_sem,
):
    layers, prompts, rows, head_size = keys_in.shape
    per_block, page_rows = outbox.shape[3], outbox.shape[4]
    heads_here = page_rows // page_size
    pages = table.shape[1]
    query_heads = queries.shape[1]
    me, row = lax.axis_index("sp"), lax.axis_index("tp")

    def head_copy(layer, step):
        other = lax.rem(row + step, tp_size)
        return pltpu.make_async_remote_copy(
            src_ref=heads_out.at[layer, row],
            dst_ref=heads_out.at[layer, row],
            send_sem=head_send_sem.at[layer, step],
            recv_sem=head_recv_sem.at[layer, step],
            device_id={"tp": other},
            device_id_type=MESH,
        )

    def block_copy(layer, step):
        other = partner(me, step, sp_size)
        return pltpu.make_async_remote_copy(
            src_ref=outbox.at[layer, other],
            dst_ref=inboxes[layer].at[me],
            send_sem=send_sem.at[layer, step],
            recv_sem=recv_sem.at[layer, step],
            device_id={"sp": other},
            device_id_type=MESH,
        )

    fetches = []
    for layer in range(layers):
        for kind, source in enumerate((keys_in, values_in)):
            fetch = pltpu.make_async_copy(
                source.at[layer], fetched.at[layer, kind], fetch_sem.at[layer, kind]
            )
            fetch.start()
            fetches.append(fetch)

    barrier = pltpu.get_barrier_semaphore()

    def greet_sp(step, carry):
        pl.semaphore_signal(
            barrier, inc=1, device_id={"sp": partner(me, step, sp_size)}, device_id_type=MESH
        )
        return carry

    half, quarter = sp_size // 2, sp_size // 4
    split = staged(sp_size)
    if split:
        place_in_line, place_in_quarter = me // quarter, me % quarter
        inner = (place_in_line + me // half) % 2
        lax.fori_loop(1, half, greet_sp, 0)

        @pl.when(inner == 1)
        def _():
            lax.fori_loop(half + quarter, sp_size, greet_sp, 0)

        greeted = half - 1 + inner * quarter
    else:
        lax.fori_loop(1, sp_size, greet_sp, 0)
        greeted = sp_size - 1
    for step in range(1, tp_size):
        pl.semaphore_signal(
            barrier, inc=1, device_id={"tp": lax.rem(row + step, tp_size)}, device_id_type=MESH
        )

    def holder_of(slot):
        def look(prompt, found):
            return jnp.where(destination[prompt] == slot, prompt, found)

        return lax.fori_loop(0, prompts, look, jnp.int32(0), unroll=prompts <= 8)

    my_len = lengths[holder_of(me)]
    for fetch in fetches:
        fetch.wait()

    def fill(step, carry):
        other = partner(me, step, sp_size)
        held = holder_of(other)
        for layer in range(layers):
            for kind in range(2):
                block = fetched[layer, kind, held]
                outbox[layer, other, kind] = block.reshape(per_block, page_rows, head_size)
        return carry

    lax.fori_loop(1, sp_size, fill, 0)
    own = holder_of(me)
    for layer in range(layers):
        for kind in range(2):
            block = fetched[layer, kind, own]
            inboxes[layer][me, kind] = block.reshape(per_block, page_rows, head_size)

    pl.semaphore_wait(barrier, greeted + tp_size - 1)

    def send_steps(layer, first, stop):
        def send(step, carry):
            block_copy(layer, turn(me, step, sp_size, layer == layers - 1 and layer > 0)).start()
            return carry

        lax.fori_loop(first, stop, send, 0)

    def pass_on(level, line):
        pl.semaphore_signal(
            far_sem.at[level], inc=1,
            device_id={"sp": line * quarter + place_in_quarter}, device_id_type=MESH,
        )

    if split:
        outward, inward = (place_in_line // 2) * 3, 3 - place_in_line

        @pl.when(inner == 1)
        def _():
            pass_on(0, inward)
            pass_on(0, outward)
            send_steps(0, 1, half + quarter)
            pl.semaphore_wait(far_sem.at[0], 1)
            pass_on(1, outward)
            send_steps(0, half + quarter, sp_size)
            for layer in range(1, layers):
                send_steps(layer, 1, sp_size)

        @pl.when(inner == 0)
        def _():
            for layer in range(layers):
                send_steps(layer, 1, half)
            pl.semaphore_wait(far_sem.at[0], 1)
            send_steps(0, half, half + quarter)
            pl.semaphore_wait(far_sem.at[1], 1)
            send_steps(0, half + quarter, sp_size)
            for layer in range(1, layers):
                send_steps(layer, half, sp_size)
    else:
        for layer in range(layers):
            send_steps(layer, 1, sp_size)

    def invert(page, carry):
        def look(position, found):
            return jnp.where(table[0, position] == page, position, found)

        inverse[page] = lax.fori_loop(0, pages, look, jnp.int32(0), unroll=pages <= 32)
        return carry

    lax.fori_loop(0, pages, invert, 0)

    groups = query_heads // heads_here
    shape = (query_heads, rows)
    column = lax.broadcasted_iota(jnp.int32, shape, 1)
    column_head, column_token = column % heads_here, column // heads_here
    same_head = lax.broadcasted_iota(jnp.int32, shape, 0) // groups == column_head
    page_token = lax.broadcasted_iota(jnp.int32, (page_rows, head_size), 0) // heads_here
    scale = head_size ** (-0.5)
    tokens = rows // heads_here

    for layer in range(layers):
        asked = queries[layer]

        def attend(step, carry):
            top, total, mixed = carry
            step = turn(me, step, sp_size, layer == layers - 1 and layer > 0)
            source = partner(me, step, sp_size, -1)

            @pl.when(step > 0)
            def _():
                block_copy(layer, step).wait_recv()

            block_keys = inboxes[layer][source, 0].reshape(rows, head_size)
            block_values = inboxes[layer][source, 1].reshape(rows, head_size)
            scores = lax.dot_general(
                asked, block_keys, (((1,), (1,)), ((), ())), preferred_element_type=jnp.float32
            ) * scale
            seen = same_head & (column_token + source * tokens < my_len)
            scores = jnp.where(seen, scores, -1e30)
            new_top = jnp.maximum(top, jnp.max(scores, axis=1, keepdims=True))
            fade = jnp.exp(top - new_top)
            weights = jnp.exp(scores - new_top)
            high = weights.astype(jnp.bfloat16)
            low = (weights - high.astype(jnp.float32)).astype(jnp.bfloat16)
            part = jnp.dot(high, block_values, preferred_element_type=jnp.float32) + jnp.dot(
                low, block_values, preferred_element_type=jnp.float32
            )
            total = total * fade + jnp.sum(weights, axis=1, keepdims=True)
            return new_top, total, mixed * fade + part

        _, total, mixed = lax.fori_loop(
            0, sp_size, attend,
            (
                jnp.full((query_heads, 1), -1e30, jnp.float32),
                jnp.zeros((query_heads, 1), jnp.float32),
                jnp.zeros((query_heads, head_size), jnp.float32),
            ),
        )
        heads_out[layer, row] = (mixed / total).astype(jnp.bfloat16)

        def place(page, carry):
            position = inverse[page]
            source, within = position // per_block, position % per_block
            inside = page_token + position * page_size < my_len
            for kind, target in enumerate((key_pages, value_pages)):
                content = inboxes[layer][source, kind, within]
                target[layer, page] = jnp.where(inside, content, jnp.zeros_like(content))
            return carry

        early = pages // 8
        lax.fori_loop(0, early, place, 0, unroll=early <= 4)
        for step in range(1, tp_size):
            head_copy(layer, step).start()
        lax.fori_loop(early, pages, place, 0, unroll=4)

    for layer in range(layers):
        def sent(step, carry):
            block_copy(layer, step).wait_send()
            return carry

        lax.fori_loop(1, sp_size, sent, 0)
    for layer in range(layers):
        for step in range(1, tp_size):
            head_copy(layer, step).wait()
        attended[layer] = heads_out[layer].reshape(tp_size * query_heads, head_size)


def write_out(*refs):
    sources, targets, sems = refs[:3], refs[3:6], refs[6]
    copies = [
        pltpu.make_async_copy(sources[i], targets[i], sems.at[i]) for i in range(3)
    ]
    for copy in copies:
        copy.start()
    for copy in copies:
        copy.wait()


def local(sp_size, tp_size, prefill_keys, prefill_values, prompt_lengths, destination, page_table, queries):
    layers, prompts, tokens, heads_here, head_size = prefill_keys.shape
    slots_here, pages = page_table.shape
    query_heads = queries.shape[2]
    page_size = tokens * sp_size // pages
    rows, page_rows = tokens * heads_here, page_size * heads_here
    per_block = tokens // page_size
    assert slots_here == 1 and per_block * page_size == tokens
    flat = (layers, prompts, rows, head_size)
    paged = (layers, pages, page_rows, head_size)
    shapes = (paged, paged, (layers, tp_size * query_heads, head_size))
    everywhere = pl.BlockSpec(memory_space=pl.ANY)
    scalars = pl.BlockSpec(memory_space=pltpu.SMEM)
    vectors = pl.BlockSpec(memory_space=pltpu.VMEM)
    boxes = (layers, sp_size, 2, per_block, page_rows, head_size)
    kind = prefill_keys.dtype
    dma = pltpu.SemaphoreType.DMA
    grant = min(60 * 1024 * 1024, 67043328 - 2 * prefill_keys.size * kind.itemsize - (1 << 20))
    results = pl.pallas_call(
        functools.partial(kernel, sp_size, tp_size, page_size),
        out_shape=tuple(pltpu.VMEM(shape, kind) for shape in shapes),
        in_specs=[scalars, scalars, scalars, vectors, everywhere, everywhere],
        out_specs=(vectors, vectors, vectors),
        scratch_shapes=[
            pltpu.VMEM((layers, 2, prompts, rows, head_size), kind),
            pltpu.VMEM(boxes, kind),
            (pltpu.VMEM(boxes[1:], kind),) * layers,
            pltpu.VMEM((layers, tp_size, query_heads, head_size), jnp.bfloat16),
            pltpu.SMEM((pages,), jnp.int32),
            dma((layers, 2)),
            dma((layers, sp_size)),
            dma((layers, sp_size)),
            dma((layers, tp_size)),
            dma((layers, tp_size)),
            pltpu.SemaphoreType.REGULAR((2,)),
        ],
        compiler_params=pltpu.CompilerParams(
            collective_id=0, has_side_effects=True, vmem_limit_bytes=grant
        ),
    )(
        prompt_lengths,
        destination,
        page_table,
        queries.reshape(layers, query_heads, head_size),
        prefill_keys.reshape(flat),
        prefill_values.reshape(flat),
    )
    key_pages, value_pages, attended = pl.pallas_call(
        write_out,
        out_shape=tuple(jax.ShapeDtypeStruct(shape, kind) for shape in shapes),
        in_specs=[vectors] * 3,
        out_specs=(everywhere,) * 3,
        scratch_shapes=[dma((3,))],
        compiler_params=pltpu.CompilerParams(vmem_limit_bytes=1 << 20),
    )(*(pltpu.with_memory_space_constraint(x, pltpu.VMEM) for x in results))
    shape = (layers, pages, page_size, heads_here, head_size)
    return (
        key_pages.reshape(shape),
        value_pages.reshape(shape),
        attended.reshape(layers, 1, tp_size * query_heads, head_size),
    )


def solution(mesh):
    placed = (
        P(None, None, "sp", "tp", None),
        P(None, None, "sp", "tp", None),
        P(),
        P(),
        P("sp", None),
        P(None, "sp", "tp", None),
    )
    return jax.shard_map(
        functools.partial(local, mesh.shape["sp"], mesh.shape["tp"]),
        mesh=mesh,
        in_specs=placed,
        out_specs=(
            P(None, "sp", None, "tp", None),
            P(None, "sp", None, "tp", None),
            P(None, "sp", None, None),
        ),
        check_vma=False,
    )
```

```python
import functools

import jax
import jax.numpy as jnp
from jax import lax
from jax.experimental import pallas as pl
from jax.experimental.pallas import tpu as pltpu
from jax.sharding import PartitionSpec as P

MESH = pl.DeviceIdType.MESH


def partner(me, step, n, way=1):
    if n & (n - 1):
        return lax.rem(me + way * step + n, n)
    total, bit = 0, 1
    while bit < n:
        total = total + ((me // bit + step // bit) % 2) * bit
        bit *= 2
    return total


def staged(n):
    return n >= 4 and not n & (n - 1)


def turn(me, step, n, last):
    if not staged(n):
        return step
    inner = (me // (n // 4) + me // (n // 2)) % 2
    swap = 1 - inner if last else inner
    crossing = step // (n // 2)
    return step + crossing * ((step + swap * (n // 4)) % (n // 2) + n // 2 - step)


def kernel(
    sp_size, tp_size, page_size,
    lengths, destination, table, queries, keys_in, values_in,
    key_pages, value_pages, attended,
    fetched, outbox, inboxes, heads_out, inverse,
    fetch_sem, send_sem, recv_sem, head_send_sem, head_recv_sem, far_sem,
):
    layers, prompts, rows, head_size = keys_in.shape
    per_block, page_rows = outbox.shape[3], outbox.shape[4]
    heads_here = page_rows // page_size
    pages = table.shape[1]
    query_heads = queries.shape[1]
    me, row = lax.axis_index("sp"), lax.axis_index("tp")

    def head_copy(layer, step):
        other = lax.rem(row + step, tp_size)
        return pltpu.make_async_remote_copy(
            src_ref=heads_out.at[layer, row],
            dst_ref=heads_out.at[layer, row],
            send_sem=head_send_sem.at[layer, step],
            recv_sem=head_recv_sem.at[layer, step],
            device_id={"tp": other},
            device_id_type=MESH,
        )

    def block_copy(layer, step):
        other = partner(me, step, sp_size)
        return pltpu.make_async_remote_copy(
            src_ref=outbox.at[layer, other],
            dst_ref=inboxes[layer].at[me],
            send_sem=send_sem.at[layer, step],
            recv_sem=recv_sem.at[layer, step],
            device_id={"sp": other},
            device_id_type=MESH,
        )

    fetches = []
    for layer in range(layers):
        for kind, source in enumerate((keys_in, values_in)):
            fetch = pltpu.make_async_copy(
                source.at[layer], fetched.at[layer, kind], fetch_sem.at[layer, kind]
            )
            fetch.start()
            fetches.append(fetch)

    barrier = pltpu.get_barrier_semaphore()

    def greet_sp(step, carry):
        pl.semaphore_signal(
            barrier, inc=1, device_id={"sp": partner(me, step, sp_size)}, device_id_type=MESH
        )
        return carry

    half, quarter = sp_size // 2, sp_size // 4
    split = staged(sp_size)
    if split:
        place_in_line, place_in_quarter = me // quarter, me % quarter
        inner = (place_in_line + me // half) % 2
        lax.fori_loop(1, half, greet_sp, 0)

        @pl.when(inner == 1)
        def _():
            lax.fori_loop(half + quarter, sp_size, greet_sp, 0)

        greeted = half - 1 + inner * quarter
    else:
        lax.fori_loop(1, sp_size, greet_sp, 0)
        greeted = sp_size - 1
    for step in range(1, tp_size):
        pl.semaphore_signal(
            barrier, inc=1, device_id={"tp": lax.rem(row + step, tp_size)}, device_id_type=MESH
        )

    def holder_of(slot):
        def look(prompt, found):
            return jnp.where(destination[prompt] == slot, prompt, found)

        return lax.fori_loop(0, prompts, look, jnp.int32(0), unroll=prompts <= 8)

    my_len = lengths[holder_of(me)]
    for fetch in fetches:
        fetch.wait()

    def fill(step, carry):
        other = partner(me, step, sp_size)
        held = holder_of(other)
        for layer in range(layers):
            for kind in range(2):
                block = fetched[layer, kind, held]
                outbox[layer, other, kind] = block.reshape(per_block, page_rows, head_size)
        return carry

    lax.fori_loop(1, sp_size, fill, 0)
    own = holder_of(me)
    for layer in range(layers):
        for kind in range(2):
            block = fetched[layer, kind, own]
            inboxes[layer][me, kind] = block.reshape(per_block, page_rows, head_size)

    pl.semaphore_wait(barrier, greeted + tp_size - 1)

    def send_steps(layer, first, stop):
        def send(step, carry):
            block_copy(layer, turn(me, step, sp_size, layer == layers - 1 and layer > 0)).start()
            return carry

        lax.fori_loop(first, stop, send, 0)

    def pass_on(level, line):
        pl.semaphore_signal(
            far_sem.at[level], inc=1,
            device_id={"sp": line * quarter + place_in_quarter}, device_id_type=MESH,
        )

    if split:
        outward, inward = (place_in_line // 2) * 3, 3 - place_in_line

        @pl.when(inner == 1)
        def _():
            pass_on(0, inward)
            pass_on(0, outward)
            send_steps(0, half, half + quarter)
            pl.semaphore_wait(far_sem.at[0], 1)
            pass_on(1, outward)
            send_steps(0, half + quarter, sp_size)
            send_steps(0, 1, half)
            for layer in range(1, layers):
                send_steps(layer, half, sp_size)
                send_steps(layer, 1, half)

        @pl.when(inner == 0)
        def _():
            send_steps(0, 1, half)
            pl.semaphore_wait(far_sem.at[0], 1)
            send_steps(0, half, half + quarter)
            pl.semaphore_wait(far_sem.at[1], 1)
            send_steps(0, half + quarter, sp_size)
            for layer in range(1, layers):
                send_steps(layer, 1, sp_size)
    else:
        for layer in range(layers):
            send_steps(layer, 1, sp_size)

    def invert(page, carry):
        def look(position, found):
            return jnp.where(table[0, position] == page, position, found)

        inverse[page] = lax.fori_loop(0, pages, look, jnp.int32(0), unroll=pages <= 32)
        return carry

    lax.fori_loop(0, pages, invert, 0)

    groups = query_heads // heads_here
    joint = 2 if sp_size >= 8 and split else 1
    shape = (query_heads, joint * rows)
    column = lax.broadcasted_iota(jnp.int32, shape, 1)
    column_head, column_token = column % heads_here, column // heads_here
    same_head = lax.broadcasted_iota(jnp.int32, shape, 0) // groups == column_head
    page_token = lax.broadcasted_iota(jnp.int32, (page_rows, head_size), 0) // heads_here
    scale = head_size ** (-0.5)
    tokens = rows // heads_here

    for layer in range(layers):
        asked = queries[layer]

        def attend(step, carry):
            top, total, mixed = carry
            step = turn(me, step * joint, sp_size, layer == layers - 1 and layer > 0)
            source = partner(me, step, sp_size, -1) // joint * joint

            @pl.when(step > 0)
            def _():
                block_copy(layer, step).wait_recv()

            for more in range(1, joint):
                block_copy(layer, step + more).wait_recv()
            both = pl.ds(source, joint)
            block_keys = inboxes[layer][both, 0].reshape(joint * rows, head_size)
            block_values = inboxes[layer][both, 1].reshape(joint * rows, head_size)
            scores = lax.dot_general(
                asked, block_keys, (((1,), (1,)), ((), ())), preferred_element_type=jnp.float32
            ) * scale
            seen = same_head & (column_token + source * tokens < my_len)
            scores = jnp.where(seen, scores, -1e30)
            new_top = jnp.maximum(top, jnp.max(scores, axis=1, keepdims=True))
            fade = jnp.exp(top - new_top)
            weights = jnp.exp(scores - new_top)
            high = weights.astype(jnp.bfloat16)
            low = (weights - high.astype(jnp.float32)).astype(jnp.bfloat16)
            part = jnp.dot(high, block_values, preferred_element_type=jnp.float32) + jnp.dot(
                low, block_values, preferred_element_type=jnp.float32
            )
            total = total * fade + jnp.sum(weights, axis=1, keepdims=True)
            return new_top, total, mixed * fade + part

        _, total, mixed = lax.fori_loop(
            0, sp_size // joint, attend,
            (
                jnp.full((query_heads, 1), -1e30, jnp.float32),
                jnp.zeros((query_heads, 1), jnp.float32),
                jnp.zeros((query_heads, head_size), jnp.float32),
            ),
        )
        heads_out[layer, row] = (mixed / total).astype(jnp.bfloat16)

        def place(page, carry):
            position = inverse[page]
            source, within = position // per_block, position % per_block
            inside = page_token + position * page_size < my_len
            for kind, target in enumerate((key_pages, value_pages)):
                content = inboxes[layer][source, kind, within]
                target[layer, page] = jnp.where(inside, content, jnp.zeros_like(content))
            return carry

        early = pages // 8
        lax.fori_loop(0, early, place, 0, unroll=early <= 4)
        for step in range(1, tp_size):
            head_copy(layer, step).start()
        lax.fori_loop(early, pages, place, 0, unroll=4)

    for layer in range(layers):
        def sent(step, carry):
            block_copy(layer, step).wait_send()
            return carry

        lax.fori_loop(1, sp_size, sent, 0)
    for layer in range(layers):
        for step in range(1, tp_size):
            head_copy(layer, step).wait()
        attended[layer] = heads_out[layer].reshape(tp_size * query_heads, head_size)


def write_out(*refs):
    sources, targets, sems = refs[:3], refs[3:6], refs[6]
    copies = [
        pltpu.make_async_copy(sources[i], targets[i], sems.at[i]) for i in range(3)
    ]
    for copy in copies:
        copy.start()
    for copy in copies:
        copy.wait()


def local(sp_size, tp_size, prefill_keys, prefill_values, prompt_lengths, destination, page_table, queries):
    layers, prompts, tokens, heads_here, head_size = prefill_keys.shape
    slots_here, pages = page_table.shape
    query_heads = queries.shape[2]
    page_size = tokens * sp_size // pages
    rows, page_rows = tokens * heads_here, page_size * heads_here
    per_block = tokens // page_size
    assert slots_here == 1 and per_block * page_size == tokens
    flat = (layers, prompts, rows, head_size)
    paged = (layers, pages, page_rows, head_size)
    shapes = (paged, paged, (layers, tp_size * query_heads, head_size))
    everywhere = pl.BlockSpec(memory_space=pl.ANY)
    scalars = pl.BlockSpec(memory_space=pltpu.SMEM)
    vectors = pl.BlockSpec(memory_space=pltpu.VMEM)
    boxes = (layers, sp_size, 2, per_block, page_rows, head_size)
    kind = prefill_keys.dtype
    dma = pltpu.SemaphoreType.DMA
    grant = min(60 * 1024 * 1024, 67043328 - 2 * prefill_keys.size * kind.itemsize - (1 << 20))
    results = pl.pallas_call(
        functools.partial(kernel, sp_size, tp_size, page_size),
        out_shape=tuple(pltpu.VMEM(shape, kind) for shape in shapes),
        in_specs=[scalars, scalars, scalars, vectors, everywhere, everywhere],
        out_specs=(vectors, vectors, vectors),
        scratch_shapes=[
            pltpu.VMEM((layers, 2, prompts, rows, head_size), kind),
            pltpu.VMEM(boxes, kind),
            (pltpu.VMEM(boxes[1:], kind),) * layers,
            pltpu.VMEM((layers, tp_size, query_heads, head_size), jnp.bfloat16),
            pltpu.SMEM((pages,), jnp.int32),
            dma((layers, 2)),
            dma((layers, sp_size)),
            dma((layers, sp_size)),
            dma((layers, tp_size)),
            dma((layers, tp_size)),
            pltpu.SemaphoreType.REGULAR((2,)),
        ],
        compiler_params=pltpu.CompilerParams(
            collective_id=0, has_side_effects=True, vmem_limit_bytes=grant
        ),
    )(
        prompt_lengths,
        destination,
        page_table,
        queries.reshape(layers, query_heads, head_size),
        prefill_keys.reshape(flat),
        prefill_values.reshape(flat),
    )
    key_pages, value_pages, attended = pl.pallas_call(
        write_out,
        out_shape=tuple(jax.ShapeDtypeStruct(shape, kind) for shape in shapes),
        in_specs=[vectors] * 3,
        out_specs=(everywhere,) * 3,
        scratch_shapes=[dma((3,))],
        compiler_params=pltpu.CompilerParams(vmem_limit_bytes=1 << 20),
    )(*(pltpu.with_memory_space_constraint(x, pltpu.VMEM) for x in results))
    shape = (layers, pages, page_size, heads_here, head_size)
    return (
        key_pages.reshape(shape),
        value_pages.reshape(shape),
        attended.reshape(layers, 1, tp_size * query_heads, head_size),
    )


def solution(mesh):
    placed = (
        P(None, None, "sp", "tp", None),
        P(None, None, "sp", "tp", None),
        P(),
        P(),
        P("sp", None),
        P(None, "sp", "tp", None),
    )
    return jax.shard_map(
        functools.partial(local, mesh.shape["sp"], mesh.shape["tp"]),
        mesh=mesh,
        in_specs=placed,
        out_specs=(
            P(None, "sp", None, "tp", None),
            P(None, "sp", None, "tp", None),
            P(None, "sp", None, None),
        ),
        check_vma=False,
    )
```

```python
import functools

import jax
import jax.numpy as jnp
from jax import lax
from jax.experimental import pallas as pl
from jax.experimental.pallas import tpu as pltpu
from jax.sharding import PartitionSpec as P

MESH = pl.DeviceIdType.MESH


def partner(me, step, n, way=1):
    if n & (n - 1):
        return lax.rem(me + way * step + n, n)
    total, bit = 0, 1
    while bit < n:
        total = total + ((me // bit + step // bit) % 2) * bit
        bit *= 2
    return total


def staged(n):
    return n >= 4 and not n & (n - 1)


def turn(me, step, n, last):
    if not staged(n):
        return step
    inner = (me // (n // 4) + me // (n // 2)) % 2
    swap = 1 - inner if last else inner
    crossing = step // (n // 2)
    return step + crossing * ((step + swap * (n // 4)) % (n // 2) + n // 2 - step)


def kernel(
    sp_size, tp_size, page_size,
    lengths, destination, table, queries, keys_in, values_in,
    key_pages, value_pages, attended,
    fetched, outbox, inboxes, heads_out, inverse,
    fetch_sem, send_sem, recv_sem, head_send_sem, head_recv_sem, far_sem,
):
    layers, prompts, rows, head_size = keys_in.shape
    per_block, page_rows = outbox.shape[3], outbox.shape[4]
    heads_here = page_rows // page_size
    pages = table.shape[1]
    query_heads = queries.shape[1]
    me, row = lax.axis_index("sp"), lax.axis_index("tp")

    def head_copy(layer, step):
        other = lax.rem(row + step, tp_size)
        return pltpu.make_async_remote_copy(
            src_ref=heads_out.at[layer, row],
            dst_ref=heads_out.at[layer, row],
            send_sem=head_send_sem.at[layer, step],
            recv_sem=head_recv_sem.at[layer, step],
            device_id={"tp": other},
            device_id_type=MESH,
        )

    def block_copy(layer, step):
        other = partner(me, step, sp_size)
        return pltpu.make_async_remote_copy(
            src_ref=outbox.at[layer, other],
            dst_ref=inboxes[layer].at[me],
            send_sem=send_sem.at[layer, step],
            recv_sem=recv_sem.at[layer, step],
            device_id={"sp": other},
            device_id_type=MESH,
        )

    fetches = []
    for layer in range(layers):
        for kind, source in enumerate((keys_in, values_in)):
            fetch = pltpu.make_async_copy(
                source.at[layer], fetched.at[layer, kind], fetch_sem.at[layer, kind]
            )
            fetch.start()
            fetches.append(fetch)

    barrier = pltpu.get_barrier_semaphore()

    def greet_sp(step, carry):
        pl.semaphore_signal(
            barrier, inc=1, device_id={"sp": partner(me, step, sp_size)}, device_id_type=MESH
        )
        return carry

    half, quarter = sp_size // 2, sp_size // 4
    split = staged(sp_size)
    if split:
        place_in_line, place_in_quarter = me // quarter, me % quarter
        inner = (place_in_line + me // half) % 2
        lax.fori_loop(1, half, greet_sp, 0)

        @pl.when(inner == 1)
        def _():
            lax.fori_loop(half + quarter, sp_size, greet_sp, 0)

        greeted = half - 1 + inner * quarter
    else:
        lax.fori_loop(1, sp_size, greet_sp, 0)
        greeted = sp_size - 1
    for step in range(1, tp_size):
        pl.semaphore_signal(
            barrier, inc=1, device_id={"tp": lax.rem(row + step, tp_size)}, device_id_type=MESH
        )

    def holder_of(slot):
        def look(prompt, found):
            return jnp.where(destination[prompt] == slot, prompt, found)

        return lax.fori_loop(0, prompts, look, jnp.int32(0), unroll=prompts <= 8)

    my_len = lengths[holder_of(me)]
    for fetch in fetches:
        fetch.wait()

    def fill(step, carry):
        other = partner(me, step, sp_size)
        held = holder_of(other)
        for layer in range(layers):
            for kind in range(2):
                block = fetched[layer, kind, held]
                outbox[layer, other, kind] = block.reshape(per_block, page_rows, head_size)
        return carry

    lax.fori_loop(1, sp_size, fill, 0)
    own = holder_of(me)
    for layer in range(layers):
        for kind in range(2):
            block = fetched[layer, kind, own]
            inboxes[layer][me, kind] = block.reshape(per_block, page_rows, head_size)

    pl.semaphore_wait(barrier, greeted + tp_size - 1)

    def send_steps(layer, first, stop):
        def send(step, carry):
            block_copy(layer, turn(me, step, sp_size, layer == layers - 1 and layer > 0)).start()
            return carry

        lax.fori_loop(first, stop, send, 0)

    def pass_on(level, line):
        pl.semaphore_signal(
            far_sem.at[level], inc=1,
            device_id={"sp": line * quarter + place_in_quarter}, device_id_type=MESH,
        )

    if split:
        outward, inward = (place_in_line // 2) * 3, 3 - place_in_line

        @pl.when(inner == 1)
        def _():
            pass_on(0, inward)
            pass_on(0, outward)
            send_steps(0, half, half + quarter)
            pl.semaphore_wait(far_sem.at[0], 1)
            pass_on(1, outward)
            send_steps(0, half + quarter, sp_size)
            send_steps(0, 1, half)
            for layer in range(1, layers):
                send_steps(layer, half, sp_size)
                send_steps(layer, 1, half)

        @pl.when(inner == 0)
        def _():
            send_steps(0, 1, half)
            pl.semaphore_wait(far_sem.at[0], 1)
            send_steps(0, half, half + quarter)
            pl.semaphore_wait(far_sem.at[1], 1)
            send_steps(0, half + quarter, sp_size)
            for layer in range(1, layers):
                send_steps(layer, 1, sp_size)
    else:
        for layer in range(layers):
            send_steps(layer, 1, sp_size)

    def invert(page, carry):
        def look(position, found):
            return jnp.where(table[0, position] == page, position, found)

        inverse[page] = lax.fori_loop(0, pages, look, jnp.int32(0), unroll=pages <= 32)
        return carry

    lax.fori_loop(0, pages, invert, 0)

    groups = query_heads // heads_here
    joint = half if split else 1
    shape = (query_heads, joint * rows)
    column = lax.broadcasted_iota(jnp.int32, shape, 1)
    column_head, column_token = column % heads_here, column // heads_here
    same_head = lax.broadcasted_iota(jnp.int32, shape, 0) // groups == column_head
    page_token = lax.broadcasted_iota(jnp.int32, (page_rows, head_size), 0) // heads_here
    scale = head_size ** (-0.5)
    tokens = rows // heads_here

    for layer in range(layers):
        asked = queries[layer]

        def attend(step, carry):
            top, total, mixed = carry
            step = step * joint
            source = partner(me, step, sp_size, -1) // joint * joint

            @pl.when(step > 0)
            def _():
                block_copy(layer, step).wait_recv()

            for more in range(1, joint):
                block_copy(layer, step + more).wait_recv()
            both = pl.ds(source, joint)
            block_keys = inboxes[layer][both, 0].reshape(joint * rows, head_size)
            block_values = inboxes[layer][both, 1].reshape(joint * rows, head_size)
            scores = lax.dot_general(
                asked, block_keys, (((1,), (1,)), ((), ())), preferred_element_type=jnp.float32
            ) * scale
            seen = same_head & (column_token + source * tokens < my_len)
            scores = jnp.where(seen, scores, -1e30)
            new_top = jnp.maximum(top, jnp.max(scores, axis=1, keepdims=True))
            fade = jnp.exp(top - new_top)
            weights = jnp.exp(scores - new_top)
            high = weights.astype(jnp.bfloat16)
            low = (weights - high.astype(jnp.float32)).astype(jnp.bfloat16)
            part = jnp.dot(high, block_values, preferred_element_type=jnp.float32) + jnp.dot(
                low, block_values, preferred_element_type=jnp.float32
            )
            total = total * fade + jnp.sum(weights, axis=1, keepdims=True)
            return new_top, total, mixed * fade + part

        _, total, mixed = lax.fori_loop(
            0, sp_size // joint, attend,
            (
                jnp.full((query_heads, 1), -1e30, jnp.float32),
                jnp.zeros((query_heads, 1), jnp.float32),
                jnp.zeros((query_heads, head_size), jnp.float32),
            ),
        )
        heads_out[layer, row] = (mixed / total).astype(jnp.bfloat16)

        def place(page, carry):
            position = inverse[page]
            source, within = position // per_block, position % per_block
            inside = page_token + position * page_size < my_len
            for kind, target in enumerate((key_pages, value_pages)):
                content = inboxes[layer][source, kind, within]
                target[layer, page] = jnp.where(inside, content, jnp.zeros_like(content))
            return carry

        early = pages // 8
        lax.fori_loop(0, early, place, 0, unroll=early <= 4)
        for step in range(1, tp_size):
            head_copy(layer, step).start()
        lax.fori_loop(early, pages, place, 0, unroll=4)

    for layer in range(layers):
        def sent(step, carry):
            block_copy(layer, step).wait_send()
            return carry

        lax.fori_loop(1, sp_size, sent, 0)
    for layer in range(layers):
        for step in range(1, tp_size):
            head_copy(layer, step).wait()
        attended[layer] = heads_out[layer].reshape(tp_size * query_heads, head_size)


def write_out(*refs):
    sources, targets, sems = refs[:3], refs[3:6], refs[6]
    copies = [
        pltpu.make_async_copy(sources[i], targets[i], sems.at[i]) for i in range(3)
    ]
    for copy in copies:
        copy.start()
    for copy in copies:
        copy.wait()


def local(sp_size, tp_size, prefill_keys, prefill_values, prompt_lengths, destination, page_table, queries):
    layers, prompts, tokens, heads_here, head_size = prefill_keys.shape
    slots_here, pages = page_table.shape
    query_heads = queries.shape[2]
    page_size = tokens * sp_size // pages
    rows, page_rows = tokens * heads_here, page_size * heads_here
    per_block = tokens // page_size
    assert slots_here == 1 and per_block * page_size == tokens
    flat = (layers, prompts, rows, head_size)
    paged = (layers, pages, page_rows, head_size)
    shapes = (paged, paged, (layers, tp_size * query_heads, head_size))
    everywhere = pl.BlockSpec(memory_space=pl.ANY)
    scalars = pl.BlockSpec(memory_space=pltpu.SMEM)
    vectors = pl.BlockSpec(memory_space=pltpu.VMEM)
    boxes = (layers, sp_size, 2, per_block, page_rows, head_size)
    kind = prefill_keys.dtype
    dma = pltpu.SemaphoreType.DMA
    grant = min(60 * 1024 * 1024, 67043328 - 2 * prefill_keys.size * kind.itemsize - (1 << 20))
    results = pl.pallas_call(
        functools.partial(kernel, sp_size, tp_size, page_size),
        out_shape=tuple(pltpu.VMEM(shape, kind) for shape in shapes),
        in_specs=[scalars, scalars, scalars, vectors, everywhere, everywhere],
        out_specs=(vectors, vectors, vectors),
        scratch_shapes=[
            pltpu.VMEM((layers, 2, prompts, rows, head_size), kind),
            pltpu.VMEM(boxes, kind),
            (pltpu.VMEM(boxes[1:], kind),) * layers,
            pltpu.VMEM((layers, tp_size, query_heads, head_size), jnp.bfloat16),
            pltpu.SMEM((pages,), jnp.int32),
            dma((layers, 2)),
            dma((layers, sp_size)),
            dma((layers, sp_size)),
            dma((layers, tp_size)),
            dma((layers, tp_size)),
            pltpu.SemaphoreType.REGULAR((2,)),
        ],
        compiler_params=pltpu.CompilerParams(
            collective_id=0, has_side_effects=True, vmem_limit_bytes=grant
        ),
    )(
        prompt_lengths,
        destination,
        page_table,
        queries.reshape(layers, query_heads, head_size),
        prefill_keys.reshape(flat),
        prefill_values.reshape(flat),
    )
    key_pages, value_pages, attended = pl.pallas_call(
        write_out,
        out_shape=tuple(jax.ShapeDtypeStruct(shape, kind) for shape in shapes),
        in_specs=[vectors] * 3,
        out_specs=(everywhere,) * 3,
        scratch_shapes=[dma((3,))],
        compiler_params=pltpu.CompilerParams(vmem_limit_bytes=1 << 20),
    )(*(pltpu.with_memory_space_constraint(x, pltpu.VMEM) for x in results))
    shape = (layers, pages, page_size, heads_here, head_size)
    return (
        key_pages.reshape(shape),
        value_pages.reshape(shape),
        attended.reshape(layers, 1, tp_size * query_heads, head_size),
    )


def solution(mesh):
    placed = (
        P(None, None, "sp", "tp", None),
        P(None, None, "sp", "tp", None),
        P(),
        P(),
        P("sp", None),
        P(None, "sp", "tp", None),
    )
    return jax.shard_map(
        functools.partial(local, mesh.shape["sp"], mesh.shape["tp"]),
        mesh=mesh,
        in_specs=placed,
        out_specs=(
            P(None, "sp", None, "tp", None),
            P(None, "sp", None, "tp", None),
            P(None, "sp", None, None),
        ),
        check_vma=False,
    )
```
